32 devices in a mesh: dp: 1 (over z), fsdp: 32 (over y, x, core).
Axes of the slice: x: 4, y: 4, z: 1, core: 2. Of those that a mesh axis runs over, the one named last changes fastest.
The devices are a block of a 4x4x8 slice.
Arguments:
- tok_ids: int32 [96, 96], P(('dp', 'fsdp'))
- grad_out: bfloat16 [96, 96, 2048], P(('dp', 'fsdp'))
- emb_table: bfloat16 [163840, 2048], P('fsdp')
- norm_gain: bfloat16 [2048], P('fsdp')
- w_query: bfloat16 [2048, 3072], P('fsdp')
- w_kv_down: bfloat16 [2048, 576], P('fsdp')
- kv_gain: bfloat16 [512], P('fsdp')
- w_kv_up: bfloat16 [512, 4096], P('fsdp')
- w_out: bfloat16 [2048, 2048], P('fsdp')
Outputs:
- output 1: bfloat16 [96, 96, 2048], P(('dp', 'fsdp'))
- output 2: bfloat16 [163840, 2048], P(('dp', 'fsdp'))
- output 3: float32 [2048], P(('dp', 'fsdp'))
- output 4: float32 [2048, 3072], P(('dp', 'fsdp'))
- output 5: float32 [2048, 576], P(('dp', 'fsdp'))
- output 6: float32 [512], P(('dp', 'fsdp'))
- output 7: float32 [512, 4096], P(('dp', 'fsdp'))
- output 8: float32 [2048, 2048], P(('dp', 'fsdp'))
All inputs are finite; a program needn't handle non-finite values.
Results may differ from the reference program's by a relative error of at most 0.0116745.
Values are sent between devices in bfloat16 or wider.
A program may use at most 768 MiB of HBM per device.

```python
import math
import jax
import jax.numpy as jnp
from jax import lax

D_MODEL = 2048
N_HEADS = 16
VOCAB_SIZE = 163840
KV_RANK = 512
BATCH_SEQS = 96
SEQ_LEN = 96
NOPE_DIM = 128
ROPE_DIM = 64
VALUE_DIM = 128
HOT_IDS = 64
ROPE_THETA = 50000.0
RMS_EPS = 1e-6
ATTN_SCALE = (NOPE_DIM + ROPE_DIM) ** -0.5 * (0.1 * math.log(32.0) + 1.0) ** 2


def draw_ids(id_key):
    tok_count = BATCH_SEQS * SEQ_LEN
    kind_key, hot_key, mid_key, any_key = jax.random.split(id_key, 4)
    id_kind = jax.random.randint(kind_key, (tok_count,), 0, 4)
    hot_draw = jax.random.randint(hot_key, (tok_count,), 0, HOT_IDS)
    mid_draw = jax.random.randint(mid_key, (tok_count,), 0, VOCAB_SIZE // 8)
    any_draw = jax.random.randint(any_key, (tok_count,), 0, VOCAB_SIZE)
    tok_list = jnp.where(id_kind == 0, hot_draw, jnp.where(id_kind == 1, mid_draw, any_draw))
    tok_list = tok_list.at[0].set(VOCAB_SIZE - 1).at[1].set(0)
    return tok_list.reshape(BATCH_SEQS, SEQ_LEN).astype(jnp.int32)


def setup_inputs(seed: int = 0, part: int = 0) -> dict:
    base_key = jax.random.key(seed)
    shared = jax.random.split(base_key, 7)
    part_keys = jax.random.split(jax.random.fold_in(base_key, part), 2)
    q_width = N_HEADS * (NOPE_DIM + ROPE_DIM)
    up_width = N_HEADS * (NOPE_DIM + VALUE_DIM)
    o_width = N_HEADS * VALUE_DIM
    emb_table = jax.random.normal(shared[0], (VOCAB_SIZE, D_MODEL), jnp.float32).astype(jnp.bfloat16)
    norm_gain = (1.0 + 0.3 * jax.random.normal(shared[1], (D_MODEL,), jnp.float32)).astype(jnp.bfloat16)
    w_query = (jax.random.normal(shared[2], (D_MODEL, q_width), jnp.float32) * D_MODEL ** -0.5).astype(jnp.bfloat16)
    w_kv_down = (jax.random.normal(shared[3], (D_MODEL, KV_RANK + ROPE_DIM), jnp.float32) * D_MODEL ** -0.5).astype(jnp.bfloat16)
    kv_gain = (1.0 + 0.3 * jax.random.normal(shared[4], (KV_RANK,), jnp.float32)).astype(jnp.bfloat16)
    w_kv_up = (jax.random.normal(shared[5], (KV_RANK, up_width), jnp.float32) * KV_RANK ** -0.5).astype(jnp.bfloat16)
    w_out = (jax.random.normal(shared[6], (o_width, D_MODEL), jnp.float32) * o_width ** -0.5).astype(jnp.bfloat16)
    tok_ids = draw_ids(part_keys[0])
    grad_out = jax.random.normal(part_keys[1], (BATCH_SEQS, SEQ_LEN, D_MODEL), jnp.float32).astype(jnp.bfloat16)
    return {'tok_ids': tok_ids, 'grad_out': grad_out, 'emb_table': emb_table, 'norm_gain': norm_gain, 'w_query': w_query, 'w_kv_down': w_kv_down, 'kv_gain': kv_gain, 'w_kv_up': w_kv_up, 'w_out': w_out}


def rms_scale(in_vals, gain_vec):
    vals_f32 = in_vals.astype(jnp.float32)
    inv_rms = lax.rsqrt(jnp.mean(vals_f32 * vals_f32, axis=-1, keepdims=True) + RMS_EPS)
    return (vals_f32 * inv_rms * gain_vec.astype(jnp.float32)).astype(jnp.bfloat16)


def rope_tables():
    positions = jnp.arange(SEQ_LEN, dtype=jnp.float32)
    inv_freq = ROPE_THETA ** (-2.0 * jnp.arange(ROPE_DIM // 2, dtype=jnp.float32) / ROPE_DIM)
    rot_angle = positions[:, None] * inv_freq[None, :]
    rot_angle = jnp.concatenate([rot_angle, rot_angle], axis=-1)
    return jnp.cos(rot_angle), jnp.sin(rot_angle)


def apply_rope(in_vals, cos_tab, sin_tab):
    half_dim = ROPE_DIM // 2
    vals_f32 = in_vals.astype(jnp.float32)
    turned = jnp.concatenate([-vals_f32[..., half_dim:], vals_f32[..., :half_dim]], axis=-1)
    return (vals_f32 * cos_tab + turned * sin_tab).astype(jnp.bfloat16)


def attend_one(q_seq, pe_seq, kv_seq):
    cos_tab, sin_tab = rope_tables()
    q_rot = apply_rope(q_seq[:, :, NOPE_DIM:], cos_tab[:, None, :], sin_tab[:, None, :])
    k_rot = apply_rope(pe_seq, cos_tab, sin_tab)
    scores = jnp.einsum('shd,thd->hst', q_seq[:, :, :NOPE_DIM].astype(jnp.float32), kv_seq[:, :, :NOPE_DIM].astype(jnp.float32))
    scores = scores + jnp.einsum('shd,td->hst', q_rot.astype(jnp.float32), k_rot.astype(jnp.float32))
    positions = jnp.arange(SEQ_LEN)
    causal = positions[:, None] >= positions[None, :]
    scores = jnp.where(causal[None, :, :], scores * ATTN_SCALE, -1e30)
    attn_probs = jax.nn.softmax(scores, axis=-1).astype(jnp.bfloat16)
    attn_mix = jnp.einsum('hst,thd->shd', attn_probs.astype(jnp.float32), kv_seq[:, :, NOPE_DIM:].astype(jnp.float32))
    return attn_mix.astype(jnp.bfloat16).reshape(SEQ_LEN, N_HEADS * VALUE_DIM)


def block_forward(rows_f32, gain_vec, w_query_f, w_down_f, kv_gain_vec, w_up_f, w_out_f):
    normed = rms_scale(rows_f32, gain_vec)
    q_proj = jnp.dot(normed.astype(jnp.float32), w_query_f, preferred_element_type=jnp.float32).astype(jnp.bfloat16)
    kv_down = jnp.dot(normed.astype(jnp.float32), w_down_f, preferred_element_type=jnp.float32).astype(jnp.bfloat16)
    latent = rms_scale(kv_down[:, :KV_RANK], kv_gain_vec)
    kv_up = jnp.dot(latent.astype(jnp.float32), w_up_f, preferred_element_type=jnp.float32).astype(jnp.bfloat16)
    seq_parts = (q_proj.reshape(BATCH_SEQS, SEQ_LEN, N_HEADS, NOPE_DIM + ROPE_DIM), kv_down[:, KV_RANK:].reshape(BATCH_SEQS, SEQ_LEN, ROPE_DIM), kv_up.reshape(BATCH_SEQS, SEQ_LEN, N_HEADS, NOPE_DIM + VALUE_DIM))
    attn_mix = lax.map(jax.checkpoint(lambda seq_item: attend_one(*seq_item)), seq_parts)
    attn_out = jnp.dot(attn_mix.reshape(BATCH_SEQS * SEQ_LEN, N_HEADS * VALUE_DIM).astype(jnp.float32), w_out_f, preferred_element_type=jnp.float32)
    return rows_f32 + attn_out


def reference(tok_ids, grad_out, emb_table, norm_gain, w_query, w_kv_down, kv_gain, w_kv_up, w_out):
    flat_ids = tok_ids.reshape(BATCH_SEQS * SEQ_LEN)
    rows_f32 = jnp.take(emb_table, flat_ids, axis=0).astype(jnp.float32)
    weight_list = tuple(weight_arr.astype(jnp.float32) for weight_arr in (norm_gain, w_query, w_kv_down, kv_gain, w_kv_up, w_out))
    out_f32, pullback = jax.vjp(block_forward, rows_f32, *weight_list)
    grad_list = pullback(grad_out.reshape(BATCH_SEQS * SEQ_LEN, D_MODEL).astype(jnp.float32))
    grad_table = jax.ops.segment_sum(grad_list[0], flat_ids, num_segments=VOCAB_SIZE).astype(jnp.bfloat16)
    block_out = out_f32.astype(jnp.bfloat16).reshape(BATCH_SEQS, SEQ_LEN, D_MODEL)
    return (block_out, grad_table, grad_list[1], grad_list[2], grad_list[3], grad_list[4], grad_list[5], grad_list[6])
```

```python
import functools
import math
import jax
import jax.numpy as jnp
from jax import lax
from jax.experimental import pallas as pl
from jax.experimental.pallas import tpu as pltpu
from jax.sharding import PartitionSpec as P

NOPE_DIM = 128
ROPE_DIM = 64
VALUE_DIM = 128
ROPE_THETA = 50000.0
RMS_EPS = 1e-6
ATTN_SCALE = (NOPE_DIM + ROPE_DIM) ** -0.5 * (0.1 * math.log(32.0) + 1.0) ** 2
ROW_DIMS = (((0,), (0,)), ((), ()))
COL_DIMS = (((1,), (1,)), ((), ()))
LANES = 128


def weight_grads_kernel(widths, up_rows, up_cut, x_ref, d_query_ref, d_down_ref, mix_ref, d_out_ref, latent_ref, d_up_ref, out_ref):
    q_width, o_width, up_cols, c_width, spare_width = widths

    def grad(rows_ref, cols):
        return lax.dot_general(rows_ref[...], cols, ROW_DIMS, preferred_element_type=jnp.float32)

    out_ref[:, :q_width] = grad(x_ref, d_query_ref[...])
    at = q_width
    out_ref[:, at:at + o_width] = grad(mix_ref, d_out_ref[...])
    at += o_width
    for cut in range(up_cut):
        piece = lax.dot_general(latent_ref[0], d_up_ref[:, cut * up_cols:(cut + 1) * up_cols], ROW_DIMS, preferred_element_type=jnp.float32)
        for d in range(piece.shape[0] // up_rows):
            low = (d * up_cut + cut) * up_rows
            out_ref[low:low + up_rows, at:at + up_cols] = piece[d * up_rows:(d + 1) * up_rows]
    at += up_cols
    tail = grad(x_ref, d_down_ref[...])
    out_ref[:, at:] = jnp.concatenate([tail, jnp.zeros((tail.shape[0], spare_width), jnp.float32)], axis=1)


def weight_grads(up_rows, up_cut, normed, d_query, d_down, mix_rows, d_out, latent, d_up):
    toks, rows = normed.shape
    widths = (d_query.shape[1], d_out.shape[1], d_up.shape[1] // up_cut, d_down.shape[1])
    widths += (-sum(widths) % 1024,)
    block = min(256, rows)
    steps = rows // block
    kv_block = latent.shape[1] // steps
    latent = latent.reshape(toks, steps, kv_block).transpose(1, 0, 2)
    whole = lambda a: pl.BlockSpec(a.shape, lambda i: (0, 0))
    cols = pl.BlockSpec((toks, block), lambda i: (0, i))
    return pl.pallas_call(
        functools.partial(weight_grads_kernel, widths, up_rows, up_cut),
        out_shape=jax.ShapeDtypeStruct((rows, sum(widths)), jnp.float32),
        grid=(steps,),
        in_specs=[cols, whole(d_query), whole(d_down), cols, whole(d_out), pl.BlockSpec((1, toks, kv_block), lambda i: (i, 0, 0)), whole(d_up)],
        out_specs=pl.BlockSpec((block, sum(widths)), lambda i: (i, 0)),
        compiler_params=pltpu.CompilerParams(vmem_limit_bytes=48_000_000),
        cost_estimate=pl.CostEstimate(flops=2 * toks * rows * sum(widths), bytes_accessed=4 * rows * sum(widths), transcendentals=0),
        name='weight_grads',
    )(normed, d_query, d_down, mix_rows, d_out, latent, d_up)


def rms_scale(in_vals, gain_vec):
    vals_f32 = in_vals.astype(jnp.float32)
    inv_rms = lax.rsqrt(jnp.mean(vals_f32 * vals_f32, axis=-1, keepdims=True) + RMS_EPS)
    return (vals_f32 * inv_rms * gain_vec).astype(jnp.bfloat16)


def rope_tables(seq_len):
    positions = jnp.arange(seq_len, dtype=jnp.float32)
    inv_freq = ROPE_THETA ** (-2.0 * jnp.arange(ROPE_DIM // 2, dtype=jnp.float32) / ROPE_DIM)
    rot_angle = positions[:, None] * inv_freq[None, :]
    rot_angle = jnp.concatenate([rot_angle, rot_angle], axis=-1)
    return jnp.cos(rot_angle), jnp.sin(rot_angle)


def apply_rope(in_vals, cos_tab, sin_tab):
    half_dim = ROPE_DIM // 2
    vals_f32 = in_vals.astype(jnp.float32)
    turned = jnp.concatenate([-vals_f32[..., half_dim:], vals_f32[..., :half_dim]], axis=-1)
    return (vals_f32 * cos_tab + turned * sin_tab).astype(jnp.bfloat16)


def attend_local(q_proj, pe_raw, kv_up):
    seq_len = q_proj.shape[1]
    cos_tab, sin_tab = rope_tables(seq_len)
    q_rot = apply_rope(q_proj[..., NOPE_DIM:], cos_tab[:, None, :], sin_tab[:, None, :])
    k_rot = apply_rope(pe_raw, cos_tab, sin_tab)
    scores = jnp.einsum('bshd,bthd->bhst', q_proj[..., :NOPE_DIM], kv_up[..., :NOPE_DIM], preferred_element_type=jnp.float32)
    scores = scores + jnp.einsum('bshd,btd->bhst', q_rot, k_rot, preferred_element_type=jnp.float32)
    positions = jnp.arange(seq_len)
    causal = positions[:, None] >= positions[None, :]
    scores = jnp.where(causal, scores * ATTN_SCALE, -1e30)
    attn_probs = jax.nn.softmax(scores, axis=-1).astype(jnp.bfloat16)
    attn_mix = jnp.einsum('bhst,bthd->bshd', attn_probs, kv_up[..., NOPE_DIM:], preferred_element_type=jnp.float32)
    return attn_mix.astype(jnp.bfloat16)


def solution(mesh):
    tok_spec = P(('dp', 'fsdp'), None)
    seq_spec = P(('dp', 'fsdp'), None, None)
    part_vec = P(('dp', 'fsdp'))
    vec_spec = P('fsdp')
    mat_spec = P('fsdp', None)
    n = mesh.shape['fsdp']

    def device_step(tok_ids, grad_out, emb_table, norm_gain, w_query, w_kv_down, kv_gain, w_kv_up, w_out):
        seq_count, seq_len = tok_ids.shape
        vocab, d_model = emb_table.shape
        toks = seq_count * seq_len
        me = lax.axis_index('fsdp')
        d_rows_w, q_width = w_query.shape
        c_width = w_kv_down.shape[1]
        up_rows, up_width = w_kv_up.shape
        kv_rank = up_rows * n
        gain_len, kv_gain_len = norm_gain.shape[0], kv_gain.shape[0]
        up_cut = d_rows_w // up_rows
        up_cols = up_width // up_cut
        grad_rows = grad_out.reshape(toks, d_model)

        o_width = w_out.shape[1]
        o_end = q_width + o_width
        up_end = o_end + up_cols
        down_end = up_end + c_width
        w_query_full, w_down_full, w_up_full, w_out_full = (lax.all_gather(shard, 'fsdp', tiled=True) for shard in (w_query, w_kv_down, w_kv_up, w_out))

        def to_all(parts):
            return lax.all_gather(jnp.concatenate(parts), 'fsdp')

        padded = -(-toks // LANES) * LANES
        ids_f32 = jnp.concatenate([tok_ids.reshape(toks).astype(jnp.float32), jnp.zeros((padded - toks,), jnp.float32)])
        spread_all = to_all([ids_f32, norm_gain.astype(jnp.float32), kv_gain.astype(jnp.float32)])
        all_ids = spread_all[:, :toks].reshape(n * toks).astype(jnp.int32)
        gain_vec = spread_all[:, padded:padded + gain_len].reshape(n * gain_len)
        kv_gain_vec = spread_all[:, padded + gain_len:padded + gain_len + kv_gain_len].reshape(n * kv_gain_len)

        local_ids = all_ids - me * vocab
        is_owned = (local_ids >= 0) & (local_ids < vocab)
        picked = jnp.take(emb_table, jnp.where(is_owned, local_ids, 0), axis=0)
        picked = jnp.where(is_owned[:, None], picked, jnp.zeros((), picked.dtype))
        w_query_full, w_down_full, w_up_full, w_out_full, to_send = lax.optimization_barrier((w_query_full, w_down_full, w_up_full, w_out_full, picked))
        got = lax.psum_scatter(to_send, 'fsdp', scatter_dimension=0, tiled=True)
        got, late_grads = lax.optimization_barrier((got, grad_rows))
        all_d_out = lax.all_gather(late_grads, 'fsdp', tiled=True)
        rows_f32 = got.astype(jnp.float32)

        normed, norm_pull = jax.vjp(rms_scale, rows_f32, gain_vec)
        kv_down = jnp.dot(normed, w_down_full, preferred_element_type=jnp.float32).astype(jnp.bfloat16)
        q_proj = jnp.dot(normed, w_query_full, preferred_element_type=jnp.float32).astype(jnp.bfloat16)
        latent, latent_pull = jax.vjp(rms_scale, kv_down[:, :kv_rank], kv_gain_vec)
        kv_up = jnp.dot(latent, w_up_full, preferred_element_type=jnp.float32).astype(jnp.bfloat16)
        attn_mix, attn_pull = jax.vjp(attend_local, q_proj.reshape(seq_count, seq_len, -1, NOPE_DIM + ROPE_DIM), kv_down[:, kv_rank:].reshape(seq_count, seq_len, ROPE_DIM), kv_up.reshape(seq_count, seq_len, -1, NOPE_DIM + VALUE_DIM))
        mix_rows = attn_mix.reshape(toks, -1)
        out_f32 = rows_f32 + jnp.dot(mix_rows, w_out_full, preferred_element_type=jnp.float32)
        d_mix = lax.dot_general(grad_rows, w_out_full, COL_DIMS, preferred_element_type=jnp.float32).astype(jnp.bfloat16)
        d_query, d_pe, d_up = attn_pull(d_mix.reshape(attn_mix.shape))
        d_query = d_query.reshape(toks, -1)
        d_up = d_up.reshape(toks, -1)
        d_latent = lax.dot_general(d_up, w_up_full, COL_DIMS, preferred_element_type=jnp.float32).astype(jnp.bfloat16)
        d_ckv, d_kv_gain = latent_pull(d_latent)
        d_down = jnp.concatenate([d_ckv, d_pe.reshape(toks, ROPE_DIM)], axis=1)
        d_normed = lax.dot_general(d_query, w_query_full, COL_DIMS, preferred_element_type=jnp.float32)
        d_normed = d_normed + lax.dot_general(d_down, w_down_full, COL_DIMS, preferred_element_type=jnp.float32)
        d_normed = d_normed.astype(jnp.bfloat16)
        _, d_gain = norm_pull(d_normed)
        late_normed, all_d_out = lax.optimization_barrier((d_normed, all_d_out))
        all_d_normed = lax.all_gather(late_normed, 'fsdp', tiled=True)
        inv_rms = lax.rsqrt(jnp.mean(rows_f32 * rows_f32, axis=-1) + RMS_EPS)
        pull = inv_rms * inv_rms * inv_rms * jnp.mean(rows_f32 * d_normed.astype(jnp.float32) * gain_vec, axis=-1)
        pad_toks = jnp.zeros((padded - toks,), jnp.float32)
        scales = to_all([inv_rms, pad_toks, pull, pad_toks])

        d_w_cat = weight_grads(up_rows, up_cut, normed, d_query, d_down, mix_rows, grad_rows, latent, d_up)
        small = lax.psum_scatter(jnp.concatenate([d_gain.reshape(n, gain_len), d_kv_gain.reshape(n, kv_gain_len)], axis=1).reshape(-1), 'fsdp', scatter_dimension=0, tiled=True)
        d_w_cat, all_d_normed, scales, small = lax.optimization_barrier((d_w_cat, all_d_normed, scales, small))
        d_w_shard = lax.psum_scatter(d_w_cat, 'fsdp', scatter_dimension=0, tiled=True)

        all_inv = scales[:, :toks].reshape(n * toks, 1)
        all_pull = scales[:, padded:padded + toks].reshape(n * toks, 1)
        token_grads = all_d_normed.astype(jnp.float32) * gain_vec * all_inv - picked.astype(jnp.float32) * all_pull + all_d_out.astype(jnp.float32)
        grad_table = jax.ops.segment_sum(token_grads, jnp.where(is_owned, local_ids, vocab), num_segments=vocab).astype(jnp.bfloat16)

        d_w_up_shard = d_w_shard[:, o_end:up_end].reshape(up_cut, up_rows, up_cols).transpose(1, 0, 2).reshape(up_rows, up_width)
        return (
            out_f32.astype(jnp.bfloat16).reshape(seq_count, seq_len, d_model),
            grad_table,
            small[:gain_len],
            d_w_shard[:, :q_width],
            d_w_shard[:, up_end:down_end],
            small[gain_len:gain_len + kv_gain_len],
            d_w_up_shard,
            d_w_shard[:, q_width:o_end],
        )

    return jax.shard_map(device_step, mesh=mesh, in_specs=(tok_spec, seq_spec, mat_spec, vec_spec, mat_spec, mat_spec, vec_spec, mat_spec, mat_spec), out_specs=(seq_spec, tok_spec, part_vec, tok_spec, tok_spec, part_vec, tok_spec, tok_spec), check_vma=False)
```
